32 devices in a mesh: expert: 16 (over z, y, core), dp: 2 (over x).
Axes of the slice: x: 2, y: 2, z: 4, core: 2. Of those that a mesh axis runs over, the one named last changes fastest.
Arguments:
- tokens: bfloat16 [4096, 2048], P(('dp', 'expert')), parts along dimension 0, may hold values from -6 to 6
- experts_of: int32 [4096, 8], P(('dp', 'expert')), parts along dimension 0, may hold values from 0 to 15, all different within a row; in each aligned block of 128 rows (0 to 127, 128 to 255, ...) at most 80 rows name the same one
- gate_prob: float32 [4096, 8], P(('dp', 'expert')), parts along dimension 0, may hold values from 0.05 to 0.5
- gain: float32 [2048], replicated, may hold values from 0.25 to 1.75
- w_gate_up: bfloat16 [16, 2048, 1536], P('expert'), may hold values from -0.125 to 0.125
- w_down: bfloat16 [16, 768, 2048], P('expert'), may hold values from -0.21875 to 0.21875
Outputs:
- mixed: bfloat16 [4096, 2048], P(('dp', 'expert')), parts along dimension 0
The draws below stay inside these ranges and needn't reach their ends.
There are 2 independent parts, one for each index of `dp`. The reference program is written for one: setup_inputs(seed, part) draws one part's arguments, and reference() takes and returns one part's arrays. A program takes and returns all parts, laid end to end along the dimension named above; an argument that names none is the same for every part. Nothing has to cross between parts.
Inputs may be any that keep to these rules, and one draw needn't show every extreme that they name: `experts_of`: within each token the 8 experts differ; among the rows of one device no expert is named by more than 80 rows, a bound that some block reaches.
All inputs are finite; a program needn't handle non-finite values.
Results may differ from the reference program's by a relative error of at most 0.0052.
Values may be sent and summed in bfloat16 or wider, within the bound.
No kernel may reach another device: no remote copies, remote signals or barrier semaphores. Data moves between devices by JAX's collectives and lax.ppermute only.
A program may use at most 128 MiB of HBM per device.

```python
import math
import jax
import jax.numpy as jnp
import numpy as np
from jax import lax

D = 2048
FF = 768
TOP = 8
TOK_DEV = 128
EXPERTS = 16
CAP = 80
TOKENS = 2048
N_EXPERT = 16


def block_scale(key, shape, pieces, low, top_value):
    level = 1.0
    for dim, blocks in pieces:
        heights = jax.random.uniform(jax.random.fold_in(jax.random.fold_in(key, 6), dim), (blocks,), jnp.float32, low / len(pieces), top_value / len(pieces))
        level = level * jnp.repeat(jnp.exp(heights), shape[dim] // blocks).reshape((-1,) + (1,) * (len(shape) - 1 - dim))
    return level


def deal_out(rng, own, number, rows, count, top, limit, slope):
    sequence = jax.random.permutation(rng, count)
    heavy_load, ordinary = load_shares(count, rows * top, limit, slope, True), load_shares(count, rows * top, limit, slope, False)
    places = jnp.arange(count)

    def named(lengths, rotation):
        used = int((lengths > 0).sum())
        fixed = max(1, used // 4)
        shifted = fixed + (places - fixed + rotation * (used - fixed)) % max(1, count - fixed)
        return jnp.zeros((count,), jnp.int32).at[sequence[jnp.where(places < fixed, places, shifted)]].set(jnp.asarray(lengths, jnp.int32))

    lengths = jnp.where(number % 4 == 0, named(heavy_load, number // 4), named(ordinary, number - number // 4 - 1))
    mixed = jax.random.permutation(jax.random.fold_in(own, 3), count)
    giver, receiver = mixed[0:count // 2 * 2:2], mixed[1:count // 2 * 2:2]
    room = jnp.minimum(lengths[giver] - 1, limit - lengths[receiver]) // 2
    room = jnp.where((giver == sequence[0]) | (receiver == sequence[0]) | (lengths[receiver] == 0), 0, jnp.maximum(room, 0))
    shifted = jax.random.randint(jax.random.fold_in(own, 4), (count // 2,), 0, 1 << 20) % (room + 1)
    lengths = lengths.at[giver].add(-shifted).at[receiver].add(shifted)
    items = jnp.searchsorted(jnp.cumsum(lengths), jnp.arange(rows * top), side="right").astype(jnp.int32)
    table = items.reshape(top, rows).T
    table = table[jax.random.permutation(jax.random.fold_in(own, 1), rows)]
    rotation = jax.random.randint(jax.random.fold_in(own, 2), (rows, 1), 0, top)
    return jnp.take_along_axis(table, (jnp.arange(top)[None, :] + rotation) % top, axis=1)


def load_shares(amount, total, limit, skew, full):
    weights = [(1 << 20) // math.isqrt(standing ** skew) + 1 for standing in range(1, amount + 1)]
    largest = limit if full else min(limit, max(-(-total // amount), total * weights[0] // sum(weights)))
    least = 1 if total - largest >= amount - 1 else 0
    holding, surplus = [largest] + [least] * (amount - 1), total - largest - least * (amount - 1)
    while surplus > 0:
        movable = [i for i in range(1, amount) if holding[i] < largest] or [i for i in range(1, amount) if holding[i] < limit]
        mass, budget = sum([weights[i] for i in movable]), surplus
        for i in movable:
            extra = min(limit - holding[i], max(1, budget * weights[i] // mass), surplus)
            holding[i] = holding[i] + extra
            surplus = surplus - extra
    return np.array(holding)


def centred(own_key, dims, scale, most, split=(), held_as=jnp.bfloat16):
    array = jax.random.normal(own_key, dims, jnp.float32) * scale
    if len(split) > 0:
        array = block_scale(own_key, dims, split, -0.22, 0.18) * array
    return jnp.clip(array, min=-most, max=most).astype(held_as)


def setup_inputs(seed: int = 0, part: int = 0) -> dict:
    seeds = jax.random.split(jax.random.key(seed), 7)
    part_splits = jax.random.split(jax.random.fold_in(seeds[6], part), 7)
    tokens = centred(part_splits[0], (TOKENS, D), 1.0, 6.0, ((0, 16),))
    experts_of_keys = jax.random.split(jax.random.fold_in(part_splits[1], 1), TOKENS // TOK_DEV)
    experts_of_turns = jax.random.permutation(jax.random.fold_in(part_splits[1], 3), TOKENS // TOK_DEV)
    experts_of = jax.vmap(lambda own, number: deal_out(jax.random.fold_in(part_splits[1], 2), own, number, TOK_DEV, EXPERTS, TOP, CAP, 2))(experts_of_keys, experts_of_turns).reshape((TOKENS, TOP))
    gate_prob = jnp.clip(jnp.exp(math.log(0.5) - 2.3025851 * jax.random.uniform(part_splits[2], (TOKENS, TOP), jnp.float32) ** block_scale(part_splits[2], (TOKENS, TOP), ((0, 16),), -0.2, 0.2)), 0.05, 0.5)
    gain = jnp.clip(1.0 + 0.15 * jax.random.normal(seeds[3], (D,), jnp.float32), 0.25, 1.75)
    w_gate_up = centred(seeds[4], (EXPERTS, D, 2 * FF), D ** -0.5, 0.125, ((0, 16),))
    w_down = centred(seeds[5], (EXPERTS, FF, D), FF ** -0.5, 0.21875, ((0, 16),))
    return {"tokens": tokens, "experts_of": experts_of, "gate_prob": gate_prob, "gain": gain, "w_gate_up": w_gate_up, "w_down": w_down}


def reference(tokens, experts_of, gate_prob, gain, w_gate_up, w_down):
    x_wide = tokens.astype(jnp.float32)
    scale = lax.rsqrt(lax.optimization_barrier(jnp.mean(x_wide * x_wide, axis=-1, keepdims=True)) + 1e-06)
    normed = (x_wide * scale * gain).astype(jnp.bfloat16)
    flat = experts_of.reshape(N_EXPERT, TOK_DEV * TOP)
    onehot = (flat[:, :, None] == jnp.arange(EXPERTS, dtype=jnp.int32)).astype(jnp.int32)
    rank = lax.optimization_barrier(jnp.sum((jnp.cumsum(onehot, axis=1) - onehot) * onehot, axis=2))
    source = jnp.arange(N_EXPERT, dtype=jnp.int32)[:, None]
    per_expert = N_EXPERT * CAP
    slot = (flat * per_expert + source * CAP + rank).reshape(-1).astype(jnp.int32)
    token_of = (jnp.arange(TOKENS * TOP, dtype=jnp.int32) // TOP).astype(jnp.int32)
    owner = jnp.full((EXPERTS * per_expert,), TOKENS, jnp.int32).at[slot].set(token_of)
    weight_of = jnp.zeros((EXPERTS * per_expert,), jnp.float32).at[slot].set(gate_prob.reshape(-1).astype(jnp.float32))
    padded = jnp.concatenate([normed, jnp.zeros((1, D), jnp.bfloat16)], axis=0)

    def serve(total, index):
        start = (index * per_expert).astype(jnp.int32)
        rows_id = lax.dynamic_slice_in_dim(owner, start, per_expert)
        weights = lax.dynamic_slice_in_dim(weight_of, start, per_expert)
        rows = padded[rows_id]
        hidden = jnp.dot(rows, w_gate_up[index], preferred_element_type=jnp.float32)
        act = (jax.nn.silu(hidden[:, :FF]) * hidden[:, FF:]).astype(jnp.bfloat16)
        out_rows = jnp.dot(act, w_down[index], preferred_element_type=jnp.float32).astype(jnp.bfloat16)
        total = total.at[rows_id].add(weights[:, None] * out_rows.astype(jnp.float32), mode='drop')
        return (total, None)
    total, _ = lax.scan(serve, jnp.zeros((TOKENS, D), jnp.float32), jnp.arange(EXPERTS, dtype=jnp.int32))
    return (x_wide + total).astype(jnp.bfloat16)
```

```python
import jax
import jax.numpy as jnp
from jax import lax
from jax.sharding import PartitionSpec as P


def expert(rows, proj_in, proj_out):
    units = proj_out.shape[0]
    hidden = jnp.dot(rows, proj_in, preferred_element_type=jnp.float32)
    act = (jax.nn.silu(hidden[:, :units]) * hidden[:, units:]).astype(jnp.bfloat16)
    return jnp.dot(act, proj_out, preferred_element_type=jnp.float32)


def normalize(tokens, gain):
    x_wide = tokens.astype(jnp.float32)
    scale = lax.rsqrt(jnp.mean(x_wide * x_wide, axis=-1, keepdims=True) + 1e-06)
    return (x_wide * scale * gain).astype(jnp.bfloat16)


def gathered(tokens, experts_of, gate_prob, gain, w_gate_up, w_down):
    count = lax.axis_size("expert")
    me = lax.axis_index("expert")
    tok_rows, width = tokens.shape

    def hop(a, s):
        return lax.ppermute(a, "expert", [(i, i ^ s) for i in range(count)])

    normed = normalize(tokens, gain)
    far = [4 * d for d in range(count // 4 - 1, 0, -1)]
    column = {0: normed}
    for d in far:
        column[d] = hop(normed, d)
    blocks = {}
    for d in [0] + far:
        blocks[d] = column[d]
        blocks[d + 2] = hop(column[d], 2)
        for s in (d, d + 2):
            blocks[s + 1] = hop(blocks[s], 1)

    chosen = experts_of[:, :, None] == jnp.arange(count, dtype=jnp.int32)
    gates = jnp.sum(jnp.where(chosen, gate_prob[:, :, None], 0.0), axis=1)
    gates = lax.all_to_all(gates.T, "expert", split_axis=0, concat_axis=0, tiled=True)
    gates = jnp.take(gates, me ^ jnp.arange(count, dtype=jnp.int32), axis=0)

    total = tokens.astype(jnp.float32)
    for d in far + [0]:
        rows = jnp.concatenate([blocks[d + s] for s in range(4)], axis=0)
        out = expert(rows, w_gate_up[0], w_down[0])
        out = (out * gates[d : d + 4].reshape(-1, 1)).astype(jnp.bfloat16)
        out = out.reshape(4, tok_rows, width)
        pair = []
        for s in (2, 0):
            got = hop(out[s + 1], 1)
            pair.append(out[s].astype(jnp.float32) + got.astype(jnp.float32))
        got = hop(pair[0].astype(jnp.bfloat16), 2)
        mine = pair[1] + got.astype(jnp.float32)
        if d:
            mine = hop(mine.astype(jnp.bfloat16), d).astype(jnp.float32)
        total = total + mine
    return total.astype(jnp.bfloat16)


def exchanged(tokens, experts_of, gate_prob, gain, w_gate_up, w_down):
    count = lax.axis_size("expert")
    tok_rows, width = tokens.shape
    chosen = experts_of.shape[1]
    capacity = (5 * tok_rows * chosen + 4 * count - 1) // (4 * count)
    x_wide = tokens.astype(jnp.float32)
    normed = normalize(tokens, gain)
    flat = experts_of.reshape(-1)
    onehot = (flat[:, None] == jnp.arange(count, dtype=jnp.int32)).astype(jnp.int32)
    rank = jnp.sum((jnp.cumsum(onehot, axis=0) - onehot) * onehot, axis=1)
    slot = flat * capacity + rank
    token_of = jnp.arange(tok_rows * chosen, dtype=jnp.int32) // chosen
    owner = jnp.full((count * capacity,), tok_rows, jnp.int32).at[slot].set(token_of)
    weight_of = jnp.zeros((count * capacity,), jnp.float32).at[slot].set(gate_prob.reshape(-1))
    padded = jnp.concatenate([normed, jnp.zeros((1, width), jnp.bfloat16)], axis=0)
    outgoing = padded[owner].reshape(count, capacity, width)
    rows = lax.all_to_all(outgoing, "expert", split_axis=0, concat_axis=0, tiled=True)
    out_rows = expert(rows.reshape(count * capacity, width), w_gate_up[0], w_down[0])
    out_rows = out_rows.astype(jnp.bfloat16).reshape(count, capacity, width)
    returned = lax.all_to_all(out_rows, "expert", split_axis=0, concat_axis=0, tiled=True)
    returned = returned.reshape(count * capacity, width).astype(jnp.float32)
    total = (
        jnp.zeros((tok_rows + 1, width), jnp.float32).at[owner].add(weight_of[:, None] * returned)
    )
    return (x_wide + total[:tok_rows]).astype(jnp.bfloat16)


def body(tokens, experts_of, *rest):
    count = lax.axis_size("expert")
    dense = count <= 2 * experts_of.shape[1] and count % 8 == 0 and count & (count - 1) == 0
    return (gathered if dense else exchanged)(tokens, experts_of, *rest)


def solution(mesh):
    return jax.shard_map(
        body,
        mesh=mesh,
        in_specs=(
            P(("dp", "expert"), None),
            P(("dp", "expert"), None),
            P(("dp", "expert"), None),
            P(),
            P("expert", None, None),
            P("expert", None, None),
        ),
        out_specs=P(("dp", "expert"), None),
        check_vma=False,
    )
```

```python
import jax
import jax.numpy as jnp
from jax import lax
from jax.sharding import PartitionSpec as P


def expert(rows, proj_in, proj_out):
    units = proj_out.shape[0]
    hidden = jnp.dot(rows, proj_in, preferred_element_type=jnp.float32)
    act = (jax.nn.silu(hidden[:, :units]) * hidden[:, units:]).astype(jnp.bfloat16)
    return jnp.dot(act, proj_out, preferred_element_type=jnp.float32)


def normalize(tokens, gain):
    x_wide = tokens.astype(jnp.float32)
    scale = lax.rsqrt(jnp.mean(x_wide * x_wide, axis=-1, keepdims=True) + 1e-06)
    return (x_wide * scale * gain).astype(jnp.bfloat16)


def gathered(tokens, experts_of, gate_prob, gain, w_gate_up, w_down):
    count = lax.axis_size("expert")
    tok_rows, width = tokens.shape
    half = tok_rows // 2
    wide, narrow = jnp.float32, jnp.bfloat16
    lanes = 3 * count + -3 * count % 128
    lane = lax.broadcasted_iota(jnp.int32, (lanes, 128), 0)
    mine = (lane % count == lax.axis_index("expert")) & (lane < 3 * count)
    mine = mine.astype(narrow)

    def hop(a, s):
        return lax.ppermute(a, "expert", [(i, i ^ s) for i in range(count)])

    def with_gates(normed):
        chosen = experts_of[:, :, None] == jnp.arange(count, dtype=jnp.int32)
        rest = jnp.sum(jnp.where(chosen, gate_prob[:, :, None], 0.0), axis=1)
        terms = []
        for _ in range(3):
            term = lax.reduce_precision(rest, exponent_bits=8, mantissa_bits=7)
            terms.append(term)
            rest = rest - term
        tail = jnp.concatenate(terms, axis=1).astype(narrow)
        tail = jnp.pad(tail, ((0, 0), (0, lanes - tail.shape[1])))
        return jnp.concatenate([normed, tail], axis=1)

    def serve(held):
        pair = held.shape[0]
        other = hop(held, 1)
        rows = jnp.concatenate([held[:, :width], other[:, :width]], axis=0)
        tail = jnp.concatenate([held[:, width:], other[:, width:]], axis=0)
        scale = jnp.dot(tail, mine, preferred_element_type=wide)[:, :1]
        out = (expert(rows, w_gate_up[0], w_down[0]) * scale).astype(narrow)
        got = hop(out[pair:], 1)
        return out[:pair].astype(wide) + got.astype(wide)

    sent = with_gates(normalize(tokens, gain))
    parts = {"a": slice(0, half), "b": slice(half, tok_rows)}
    far = [(d, h) for d in range(count // 4 - 1, 1, -1) for h in parts]
    near = hop(sent, 4)
    across = hop(sent, 2)
    columns = {(d, h): hop(sent[parts[h]], 4 * d) for d, h in far}
    near = jnp.concatenate([near, hop(near, 2)], axis=0)
    own = serve(jnp.concatenate([sent, across], axis=0))
    got = hop(serve(near).astype(narrow), 4)
    own = own + got.astype(wide)

    total = {h: tokens[parts[h]].astype(wide) + own[parts[h]] for h in parts}
    for d, h in far:
        held = jnp.concatenate([columns[d, h], hop(columns[d, h], 2)], axis=0)
        both = serve(held)
        got = hop(both[half:].astype(narrow), 2)
        both = (both[:half] + got.astype(wide)).astype(narrow)
        total[h] = total[h] + hop(both, 4 * d).astype(wide)
    got = hop(own[tok_rows:].astype(narrow), 2).astype(wide)
    return (jnp.concatenate([total["a"], total["b"]], axis=0) + got).astype(narrow)


def exchanged(tokens, experts_of, gate_prob, gain, w_gate_up, w_down):
    count = lax.axis_size("expert")
    tok_rows, width = tokens.shape
    chosen = experts_of.shape[1]
    capacity = (5 * tok_rows * chosen + 4 * count - 1) // (4 * count)
    x_wide = tokens.astype(jnp.float32)
    normed = normalize(tokens, gain)
    flat = experts_of.reshape(-1)
    onehot = (flat[:, None] == jnp.arange(count, dtype=jnp.int32)).astype(jnp.int32)
    rank = jnp.sum((jnp.cumsum(onehot, axis=0) - onehot) * onehot, axis=1)
    slot = flat * capacity + rank
    token_of = jnp.arange(tok_rows * chosen, dtype=jnp.int32) // chosen
    owner = jnp.full((count * capacity,), tok_rows, jnp.int32).at[slot].set(token_of)
    weight_of = jnp.zeros((count * capacity,), jnp.float32).at[slot].set(gate_prob.reshape(-1))
    padded = jnp.concatenate([normed, jnp.zeros((1, width), jnp.bfloat16)], axis=0)
    outgoing = padded[owner].reshape(count, capacity, width)
    rows = lax.all_to_all(outgoing, "expert", split_axis=0, concat_axis=0, tiled=True)
    out_rows = expert(rows.reshape(count * capacity, width), w_gate_up[0], w_down[0])
    out_rows = out_rows.astype(jnp.bfloat16).reshape(count, capacity, width)
    returned = lax.all_to_all(out_rows, "expert", split_axis=0, concat_axis=0, tiled=True)
    returned = returned.reshape(count * capacity, width).astype(jnp.float32)
    total = (
        jnp.zeros((tok_rows + 1, width), jnp.float32).at[owner].add(weight_of[:, None] * returned)
    )
    return (x_wide + total[:tok_rows]).astype(jnp.bfloat16)


def body(tokens, experts_of, *rest):
    count = lax.axis_size("expert")
    dense = count <= 2 * experts_of.shape[1] and count % 8 == 0 and count & (count - 1) == 0
    return (gathered if dense else exchanged)(tokens, experts_of, *rest)


def solution(mesh):
    return jax.shard_map(
        body,
        mesh=mesh,
        in_specs=(
            P(("dp", "expert"), None),
            P(("dp", "expert"), None),
            P(("dp", "expert"), None),
            P(),
            P("expert", None, None),
            P("expert", None, None),
        ),
        out_specs=P(("dp", "expert"), None),
        check_vma=False,
    )
```

```python
import functools

import jax
import jax.numpy as jnp
from jax import lax
from jax.experimental import pallas as pl
from jax.sharding import PartitionSpec as P


def expert(rows, proj_in, proj_out):
    units = proj_out.shape[0]
    hidden = jnp.dot(rows, proj_in, preferred_element_type=jnp.float32)
    act = (jax.nn.silu(hidden[:, :units]) * hidden[:, units:]).astype(jnp.bfloat16)
    return jnp.dot(act, proj_out, preferred_element_type=jnp.float32)


def normalize(tokens, gain):
    x_wide = tokens.astype(jnp.float32)
    scale = lax.rsqrt(jnp.mean(x_wide * x_wide, axis=-1, keepdims=True) + 1e-06)
    return (x_wide * scale * gain).astype(jnp.bfloat16)


def prepare(count, tokens, experts_of, gate_prob, gain, sent, *pieces):
    rows, width = tokens.shape
    x_wide = tokens[...].astype(jnp.float32)
    scale = lax.rsqrt(jnp.mean(x_wide * x_wide, axis=-1, keepdims=True) + 1e-06)
    normed = (x_wide * scale * gain[...]).astype(jnp.bfloat16)
    lane = lax.broadcasted_iota(jnp.int32, (sent.shape[1] - width, rows), 0)
    second, third, spare = lane >= count, lane >= 2 * count, lane >= 3 * count
    index = jnp.where(third, lane - 2 * count, jnp.where(second, lane - count, lane))
    rest = jnp.zeros(lane.shape, jnp.float32)
    for k in range(experts_of.shape[0]):
        rest += jnp.where(experts_of[k : k + 1, :] == index, gate_prob[k : k + 1, :], 0.0)
    terms = []
    for _ in range(3):
        terms.append(rest.astype(jnp.bfloat16).astype(jnp.float32))
        rest = rest - terms[-1]
    tail = jnp.where(third, terms[2], jnp.where(second, terms[1], terms[0]))
    tail = jnp.where(spare, 0.0, tail).T.astype(jnp.bfloat16)
    sent[:, :width] = normed
    sent[:, width:] = tail
    start = 0
    for piece in pieces:
        part = slice(start, start + piece.shape[0])
        piece[:, :width] = normed[part]
        piece[:, width:] = tail[part]
        start = part.stop


def gathered(tokens, experts_of, gate_prob, gain, w_gate_up, w_down):
    count = lax.axis_size("expert")
    tok_rows, width = tokens.shape
    half = tok_rows // 2
    wide, narrow = jnp.float32, jnp.bfloat16
    lanes = 3 * count + -3 * count % 128
    lane = lax.broadcasted_iota(jnp.int32, (lanes, 128), 0)
    mine = (lane % count == lax.axis_index("expert")) & (lane < 3 * count)
    mine = mine.astype(narrow)

    def hop(a, s):
        return lax.ppermute(a, "expert", [(i, i ^ s) for i in range(count)])

    def serve(held):
        pair = held.shape[0]
        other = hop(held, 1)
        rows = jnp.concatenate([held[:, :width], other[:, :width]], axis=0)
        tail = jnp.concatenate([held[:, width:], other[:, width:]], axis=0)
        scale = jnp.dot(tail, mine, preferred_element_type=wide)[:, :1]
        out = (expert(rows, w_gate_up[0], w_down[0]) * scale).astype(narrow)
        got = hop(out[pair:], 1)
        return out[:pair].astype(wide) + got.astype(wide)

    sent, *pieces = pl.pallas_call(
        functools.partial(prepare, count),
        out_shape=[
            jax.ShapeDtypeStruct((rows, width + lanes), narrow) for rows in (tok_rows, half, half)
        ],
    )(tokens, experts_of.T, gate_prob.T, gain.reshape(1, -1))
    pieces = dict(zip("ab", pieces))
    parts = {"a": slice(0, half), "b": slice(half, tok_rows)}
    far = [(d, h) for d in range(count // 4 - 1, 1, -1) for h in parts]
    near = hop(sent, 4)
    across = hop(sent, 2)
    columns = {(d, h): hop(pieces[h], 4 * d) for d, h in far}
    near = jnp.concatenate([near, hop(near, 2)], axis=0)
    own = serve(jnp.concatenate([sent, across], axis=0))
    got = hop(serve(near).astype(narrow), 4)
    own = own + got.astype(wide)

    total = {h: tokens[parts[h]].astype(wide) + own[parts[h]] for h in parts}
    for d, h in far:
        held = jnp.concatenate([columns[d, h], hop(columns[d, h], 2)], axis=0)
        both = serve(held)
        got = hop(both[half:].astype(narrow), 2)
        both = (both[:half] + got.astype(wide)).astype(narrow)
        total[h] = total[h] + hop(both, 4 * d).astype(wide)
    got = hop(own[tok_rows:].astype(narrow), 2).astype(wide)
    return (jnp.concatenate([total["a"], total["b"]], axis=0) + got).astype(narrow)


def exchanged(tokens, experts_of, gate_prob, gain, w_gate_up, w_down):
    count = lax.axis_size("expert")
    tok_rows, width = tokens.shape
    chosen = experts_of.shape[1]
    capacity = (5 * tok_rows * chosen + 4 * count - 1) // (4 * count)
    x_wide = tokens.astype(jnp.float32)
    normed = normalize(tokens, gain)
    flat = experts_of.reshape(-1)
    onehot = (flat[:, None] == jnp.arange(count, dtype=jnp.int32)).astype(jnp.int32)
    rank = jnp.sum((jnp.cumsum(onehot, axis=0) - onehot) * onehot, axis=1)
    slot = flat * capacity + rank
    token_of = jnp.arange(tok_rows * chosen, dtype=jnp.int32) // chosen
    owner = jnp.full((count * capacity,), tok_rows, jnp.int32).at[slot].set(token_of)
    weight_of = jnp.zeros((count * capacity,), jnp.float32).at[slot].set(gate_prob.reshape(-1))
    padded = jnp.concatenate([normed, jnp.zeros((1, width), jnp.bfloat16)], axis=0)
    outgoing = padded[owner].reshape(count, capacity, width)
    rows = lax.all_to_all(outgoing, "expert", split_axis=0, concat_axis=0, tiled=True)
    out_rows = expert(rows.reshape(count * capacity, width), w_gate_up[0], w_down[0])
    out_rows = out_rows.astype(jnp.bfloat16).reshape(count, capacity, width)
    returned = lax.all_to_all(out_rows, "expert", split_axis=0, concat_axis=0, tiled=True)
    returned = returned.reshape(count * capacity, width).astype(jnp.float32)
    total = (
        jnp.zeros((tok_rows + 1, width), jnp.float32).at[owner].add(weight_of[:, None] * returned)
    )
    return (x_wide + total[:tok_rows]).astype(jnp.bfloat16)


def body(tokens, experts_of, *rest):
    count = lax.axis_size("expert")
    dense = count <= 2 * experts_of.shape[1] and count % 8 == 0 and count & (count - 1) == 0
    return (gathered if dense else exchanged)(tokens, experts_of, *rest)


def solution(mesh):
    return jax.shard_map(
        body,
        mesh=mesh,
        in_specs=(
            P(("dp", "expert"), None),
            P(("dp", "expert"), None),
            P(("dp", "expert"), None),
            P(),
            P("expert", None, None),
            P("expert", None, None),
        ),
        out_specs=P(("dp", "expert"), None),
        check_vma=False,
    )
```
